512 devices in a mesh: groups: 2 (over y), inst: 16 (over z), tp: 8 (over x), rep: 2 (over core).
Axes of the slice: x: 8, y: 2, z: 16, core: 2. Of those that a mesh axis runs over, the one named last changes fastest.
The devices are a block of a 8x8x16 slice.
Arguments:
- queries: bfloat16 [32, 128, 8192], P(('groups', 'rep'), 'inst', 'tp'), parts along dimension 0, may hold values from -8 to 8, as said below
- tool_key_value: bfloat16 [32, 128, 2048], P(('groups', 'rep'), 'inst', 'tp'), parts along dimension 0, may hold values from -8 to 8, as said below
- cache: bfloat16 [32, 12288, 2048], P(('groups', 'rep'), 'inst', 'tp'), parts along dimension 0, may hold values from -6 to 6
- placed: int32 [32, 16], P(('groups', 'rep'), 'inst'), parts along dimension 0, may hold values 0 or 1
- blocks: int32 [32, 16], P(('groups', 'rep'), 'inst'), parts along dimension 0, may hold values from 1 to 6
- span_len: int32 [32], P(('groups', 'rep')), parts along dimension 0, may hold values from 32 to 128
- owner: int32 [32], P(('groups', 'rep')), parts along dimension 0, may hold values from 0 to 15, as said below
Outputs:
- attended: bfloat16 [32, 128, 8192], P(('groups', 'rep'), 'inst', 'tp'), parts along dimension 0
- owned: bfloat16 [32, 2, 128, 2048], P(('groups', 'inst'), 'rep', None, 'tp'), parts along dimension 0
The draws below stay inside these ranges and needn't reach their ends.
There are 2 independent parts, one for each index of `groups`. The reference program is written for one: setup_inputs(seed, part) draws one part's arguments, and reference() takes and returns one part's arrays. A program takes and returns all parts, laid end to end along the dimension named above; each array names one. Nothing has to cross between parts.
Inputs may be any that keep to these rules, and one draw needn't show every extreme that they name: real-valued rotated queries. `tool_key_value`: real-valued rotated keys and values. `owner`: the 8 forks of one index of rep have different owners.
All inputs are finite; a program needn't handle non-finite values. No bound on the sum of `placed` on one device may be relied on, other than what follows from the above.
Results may differ from the reference program's by a relative error of at most 0.0022.
Values may be sent and summed in bfloat16 or wider, within the bound.
No kernel may reach another device: no remote copies, remote signals or barrier semaphores. Data moves between devices by JAX's collectives and lax.ppermute only.
A program may use at most 128 MiB of HBM per device.

```python
import math
import jax
import jax.numpy as jnp
from jax import lax

QUERY_HEADS = 64
KEY_HEADS = 8
HEAD_DIM = 128
BLOCK = 128
CAPB = 6
C_DEV = 8
F_REP = 8
FORK_TOTAL = 16
TOOL_SPAN = 128
CAP = 768
CACHE_SLOTS = 12288
N_INST = 16
N_REP = 2


def draw_queries(key, part):
    own_key = jax.random.fold_in(key, 11)
    complete_shape = (FORK_TOTAL, TOOL_SPAN, QUERY_HEADS, HEAD_DIM)
    base_offset = jnp.clip(2.5 * jax.random.normal(own_key, complete_shape, jnp.float32), -8.0, 8.0)
    return base_offset.reshape(FORK_TOTAL, TOOL_SPAN, QUERY_HEADS * HEAD_DIM).astype(jnp.bfloat16)


def draw_tool_key_value(key, part):
    own_key = jax.random.fold_in(key, 13)
    complete_shape = (FORK_TOTAL, TOOL_SPAN, KEY_HEADS, 2, HEAD_DIM)
    base_offset = jnp.clip(jax.random.normal(own_key, complete_shape, jnp.float32), -6.0, 6.0)
    return base_offset.reshape(FORK_TOTAL, TOOL_SPAN, KEY_HEADS * 2 * HEAD_DIM).astype(jnp.bfloat16)


def draw_owner(key, part):
    groups_list = []
    for replica in range(FORK_TOTAL // F_REP):
        order = jax.random.permutation(jax.random.fold_in(key, 31 + replica), N_INST)
        groups_list.append(order[:F_REP].astype(jnp.int32))
    return jnp.concatenate(groups_list).astype(jnp.int32)


def with_ends(result, rng, smallest, largest):
    dims = result.shape
    index_at = [jax.random.randint(jax.random.fold_in(rng, axis), (), 0, dims[axis]) for axis in range(len(dims))]
    result = result.at[tuple(index_at)].set(smallest)
    longest = dims.index(max(dims))
    index_at[longest] = (index_at[longest] + 1) % dims[longest]
    return result.at[tuple(index_at)].set(largest)


def shard_levels(stream_key, extent, cuts, low, top_value):
    gain = 1.0
    for position, shards_of in cuts:
        heights = jax.random.uniform(jax.random.fold_in(jax.random.fold_in(stream_key, 6), position), (shards_of,), jnp.float32, low / len(cuts), top_value / len(cuts))
        gain = gain * jnp.repeat(jnp.exp(heights), extent[position] // shards_of).reshape((-1,) + (1,) * (len(extent) - 1 - position))
    return gain


def gaussian(key, dims, width, reach, cuts=(), kind=jnp.bfloat16):
    loudness = shard_levels(key, dims, cuts, -0.22, 0.18) if cuts else 1.0
    entries = jax.random.normal(key, dims, jnp.float32) * width * loudness
    return jnp.minimum(jnp.maximum(entries, -reach), reach).astype(kind)


def setup_inputs(seed: int = 0, part: int = 0) -> dict:
    seeds = jax.random.split(jax.random.key(seed), 8)
    part_keys = jax.random.split(jax.random.fold_in(seeds[7], part), 8)
    return {
        "queries": draw_queries(jax.random.fold_in(jax.random.fold_in(seeds[7], part), 71), part),
        "tool_key_value": draw_tool_key_value(jax.random.fold_in(jax.random.fold_in(seeds[7], part), 71), part),
        "cache": gaussian(part_keys[2], (FORK_TOTAL, CACHE_SLOTS, KEY_HEADS * 2 * HEAD_DIM), 1.0, 6.0, ((0, 2), (1, 16), (2, 8))),
        "placed": with_ends((jax.random.randint(part_keys[3], (FORK_TOTAL, N_INST), 0, 4) < 3).astype(jnp.int32), jax.random.fold_in(part_keys[3], 1), 0, 1),
        "blocks": with_ends(jax.random.randint(part_keys[4], (FORK_TOTAL, N_INST), 1, CAPB + 1), jax.random.fold_in(part_keys[4], 1), 1, CAPB).astype(jnp.int32),
        "span_len": with_ends(jax.random.randint(part_keys[5], (FORK_TOTAL,), TOOL_SPAN // 4, TOOL_SPAN + 1), jax.random.fold_in(part_keys[5], 1), TOOL_SPAN // 4, TOOL_SPAN).astype(jnp.int32),
        "owner": draw_owner(jax.random.fold_in(jax.random.fold_in(seeds[7], part), 71), part),
    }


def reference(queries, tool_key_value, cache, placed, blocks, span_len, owner):
    query_group_size = QUERY_HEADS // KEY_HEADS
    scaling = 1.0 / math.sqrt(HEAD_DIM)
    query_matrix = queries.reshape(FORK_TOTAL, TOOL_SPAN, KEY_HEADS, query_group_size, HEAD_DIM)
    fresh_kv_rows = tool_key_value.reshape(FORK_TOTAL, TOOL_SPAN, KEY_HEADS, 2, HEAD_DIM)
    stored_cache_rows = cache.reshape(FORK_TOTAL, CACHE_SLOTS, KEY_HEADS, 2, HEAD_DIM)
    within = jnp.arange(CAP, dtype=jnp.int32)
    tokens_all = jnp.arange(TOOL_SPAN, dtype=jnp.int32)
    causal = (tokens_all[None, :] <= tokens_all[:, None]).reshape(TOOL_SPAN, N_INST, C_DEV)

    def one_fork(fork_id):
        live_len = placed[fork_id] * blocks[fork_id] * BLOCK
        live = within[None, :] < live_len[:, None]
        mask_all = jnp.concatenate([jnp.broadcast_to(live[None], (TOOL_SPAN, N_INST, CAP)), causal], axis=2)
        mask_all = mask_all[:, None, :, :]

        def single_head(head_id):
            query = query_matrix[fork_id, :, head_id].astype(jnp.float32)
            key_old = stored_cache_rows[fork_id, :, head_id, 0].astype(jnp.float32).reshape(N_INST, CAP, HEAD_DIM)
            value_old = stored_cache_rows[fork_id, :, head_id, 1].astype(jnp.float32).reshape(N_INST, CAP, HEAD_DIM)
            key_new = fresh_kv_rows[fork_id, :, head_id, 0].astype(jnp.float32).reshape(N_INST, C_DEV, HEAD_DIM)
            value_new = fresh_kv_rows[fork_id, :, head_id, 1].astype(jnp.float32).reshape(N_INST, C_DEV, HEAD_DIM)
            key_all = jnp.concatenate([key_old, key_new], axis=1)
            value_all = jnp.concatenate([value_old, value_new], axis=1)
            score = jnp.einsum('tgd,ipd->tgip', query, key_all) * scaling
            part_max = lax.optimization_barrier(jnp.max(jnp.where(mask_all, score, -jnp.inf), axis=-1))
            safe_max = jnp.where(part_max > -jnp.inf, part_max, 0.0)
            weight = jnp.where(mask_all, jnp.exp(score - safe_max[..., None]), 0.0)
            part_total = lax.optimization_barrier(jnp.sum(weight, axis=-1))
            rounded = lax.optimization_barrier(weight.astype(jnp.bfloat16)).astype(jnp.float32)
            part_numer = jnp.einsum('tgip,ipd->tgid', rounded, value_all)
            highest = lax.optimization_barrier(jnp.max(part_max, axis=-1))
            factor = jnp.where(part_max > -jnp.inf, jnp.exp(safe_max - highest[..., None]), 0.0)
            total = lax.optimization_barrier(jnp.sum(factor * part_total, axis=-1))
            numer = lax.optimization_barrier(jnp.sum(factor[..., None] * part_numer, axis=-2))
            return numer / total[..., None]
        return lax.map(single_head, jnp.arange(KEY_HEADS, dtype=jnp.int32))
    heads_out = lax.map(one_fork, jnp.arange(FORK_TOTAL, dtype=jnp.int32))
    attended = jnp.transpose(heads_out, (0, 2, 1, 3, 4)).reshape(FORK_TOTAL, TOOL_SPAN, QUERY_HEADS * HEAD_DIM)
    valid = tokens_all[None, :] < span_len[:, None]
    attended = jnp.where(valid[:, :, None], attended, 0.0).astype(jnp.bfloat16)
    kept = jnp.where(valid[:, :, None], tool_key_value, jnp.zeros((), tool_key_value.dtype)).astype(jnp.float32)
    rep_of = jnp.arange(FORK_TOTAL, dtype=jnp.int32) // F_REP
    chosen = (owner[None, None, :] == jnp.arange(N_INST, dtype=jnp.int32)[:, None, None]) & (rep_of[None, None, :] == jnp.arange(N_REP, dtype=jnp.int32)[None, :, None])
    owned = jnp.einsum('irf,ftk->irtk', chosen.astype(jnp.float32), kept).astype(jnp.bfloat16)
    return (attended, owned)
```

```python
import functools
import math

import jax
import jax.numpy as jnp
from jax import lax
from jax.experimental import pallas as pl
from jax.experimental.pallas import tpu as pltpu
from jax.sharding import PartitionSpec as P

HEAD_DIM = 128
BLOCK = 128
STEP = 256
META = 8
CODE = 16
NEVER = -1e30
FLOOR = -2000.0
NT = (((1,), (1,)), ((), ()))
TN = (((0,), (0,)), ((), ()))


def passed_along(x, by):
    size = lax.axis_size("inst")
    return lax.ppermute(x, "inst", [(i, (i + by) % size) for i in range(size)])


def meta_rows(rows, one, two, three):
    row = lax.broadcasted_iota(jnp.int32, (rows, one.shape[1]), 0)
    return jnp.where(row == 0, one, jnp.where(row == 1, two, three))


def whole(x):
    return jnp.floor(x + 0.5)


def coded(level, mean, out, sl):
    power = jnp.ceil(jnp.log2(jnp.maximum(jnp.max(jnp.abs(mean), axis=0, keepdims=True), 1e-30)))
    steps = whole(mean * jnp.exp2(15.0 - power))
    out[:HEAD_DIM, sl] = jnp.clip(steps, -32767.0, 32767.0).astype(jnp.int32).astype(jnp.int16)
    eighths = whole(level * 8.0)
    rest = whole((level - eighths * 0.125) * 2.0**18)
    out[HEAD_DIM:, sl] = meta_rows(CODE, eighths, rest, power).astype(jnp.int32).astype(jnp.int16)


def code_part(top, total, numer, out, sl):
    held = jnp.maximum(total, 1e-30)
    coded(jnp.maximum(top + jnp.log2(held), FLOOR), numer * (1.0 / held), out, sl)


def decoded(msg, sl):
    x = msg[:, sl].astype(jnp.int32).astype(jnp.float32)
    level = x[HEAD_DIM : HEAD_DIM + 1] * 0.125 + x[HEAD_DIM + 1 : HEAD_DIM + 2] * 2.0**-18
    return level, x[:HEAD_DIM] * jnp.exp2(x[HEAD_DIM + 2 : HEAD_DIM + 3] - 15.0)


def joined(parts):
    top = functools.reduce(jnp.maximum, [p[0] for p in parts])
    total, numer = 0.0, 0.0
    for t, l, n in parts:
        by = jnp.exp2(t - top)
        total = total + by * l
        numer = numer + by * n
    return top, total, numer


def held_part(ref, sl):
    return ref[HEAD_DIM : HEAD_DIM + 1, sl], ref[HEAD_DIM + 1 : HEAD_DIM + 2, sl], ref[:HEAD_DIM, sl]


def sent_part(msg, sl):
    level, mean = decoded(msg, sl)
    return level, 1.0, mean


def part_kernel(offsets, codes, members, tokens, rows, info, *refs):
    n = len(offsets)
    q_refs, fresh_ref, kv_ref = refs[:n], refs[n], refs[n + 1]
    out_refs, s_ref, o_ref = refs[n + 2 : 2 * n + 2], refs[2 * n + 2], refs[2 * n + 3]
    forks = kv_ref.shape[0]
    cap = kv_ref.shape[1]
    lanes = n * rows
    g = pl.program_id(0)
    me = info[0]
    unit = math.log2(math.e) / math.sqrt(HEAD_DIM)

    lane = lax.broadcasted_iota(jnp.int32, (1, lanes), 1)
    first = jnp.zeros((1, lanes), jnp.int32)
    for b, off in enumerate(offsets):
        here = lax.rem(me + (off + members), members) * tokens
        first = jnp.where((lane >= b * rows) & (lane < (b + 1) * rows), here, first)
    q_token = first + lax.rem(lane, tokens)
    u = lax.broadcasted_iota(jnp.int32, (2 * tokens, lanes), 0)
    seen = (u < tokens) & (me * tokens + u <= q_token)

    def one(j, steps):
        q = jnp.concatenate([r[j, :rows] for r in q_refs], axis=0)
        fresh = fresh_ref[j]
        live = info[1 + g * forks + j]
        s_new = lax.dot_general(fresh, q, NT, preferred_element_type=jnp.float32)
        s_new = jnp.where(seen, s_new, -jnp.inf)
        top = jnp.max(s_new, axis=0, keepdims=True)
        for c in range(steps):
            at = c * STEP
            s = lax.dot_general(
                kv_ref[j, at : at + STEP, :HEAD_DIM], q, NT, preferred_element_type=jnp.float32
            )
            if c == steps - 1:
                tail = jnp.where(at + BLOCK < live, s[BLOCK:], -jnp.inf)
                s_ref[at : at + BLOCK] = s[:BLOCK]
                s_ref[at + BLOCK : at + STEP] = tail
                top = jnp.maximum(top, jnp.max(s[:BLOCK], axis=0, keepdims=True))
                top = jnp.maximum(top, jnp.max(tail, axis=0, keepdims=True))
            else:
                s_ref[at : at + STEP] = s
                top = jnp.maximum(top, jnp.max(s, axis=0, keepdims=True))
        top = jnp.maximum(top, NEVER)
        w = jnp.exp2((s_new - top) * unit)
        total = jnp.sum(w, axis=0, keepdims=True)
        w = jnp.concatenate([w[tokens:], w[:tokens]], axis=0)
        numer = lax.dot_general(fresh, w.astype(jnp.bfloat16), TN, preferred_element_type=jnp.float32)
        for c in range(steps):
            at = c * STEP
            w = jnp.exp2((s_ref[at : at + STEP] - top) * unit)
            total = total + jnp.sum(w, axis=0, keepdims=True)
            numer = numer + lax.dot_general(
                kv_ref[j, at : at + STEP, HEAD_DIM:],
                w.astype(jnp.bfloat16),
                TN,
                preferred_element_type=jnp.float32,
            )
        o_ref[j, :HEAD_DIM] = numer
        row = lax.broadcasted_iota(jnp.int32, (META, lanes), 0)
        o_ref[j, HEAD_DIM:] = jnp.where(row == 0, top * unit, total)

    def fork(j, carry):
        live = info[1 + g * forks + j]
        for steps in range(cap // STEP + 1):
            pl.when((live > (steps - 1) * STEP) & (live <= steps * STEP))(
                functools.partial(one, j, steps)
            )
        return carry

    lax.fori_loop(0, forks, fork, 0)
    for b in range(n):
        o = jnp.concatenate([o_ref[j, :, b * rows : (b + 1) * rows] for j in range(forks)], axis=1)
        if codes[b]:
            code_part(o[HEAD_DIM : HEAD_DIM + 1], o[HEAD_DIM + 1 : HEAD_DIM + 2], o[:HEAD_DIM], out_refs[b], slice(None))
        else:
            out_refs[b][...] = o


def parts_of(blocks_q, offsets, codes, info, cache, fresh, members, tokens):
    n = len(offsets)
    forks, carried, _ = blocks_q[0].shape
    rows = carried - 2 * tokens
    both = 128 // rows
    cap, width = cache.shape[1:]
    keys = cap + tokens
    lanes = n * rows
    heights = [HEAD_DIM + (CODE if c else META) for c in codes]
    return pl.pallas_call(
        functools.partial(part_kernel, offsets, codes, members, tokens, rows),
        grid_spec=pltpu.PrefetchScalarGridSpec(
            num_scalar_prefetch=1,
            grid=(forks // both,),
            in_specs=[pl.BlockSpec((both, carried, HEAD_DIM), lambda g, i: (g, 0, 0))] * n
            + [
                pl.BlockSpec((both, 2 * tokens, HEAD_DIM), lambda g, i: (g, rows // (2 * tokens), 0)),
                pl.BlockSpec((both, cap, width), lambda g, i: (g, 0, 0)),
            ],
            out_specs=[pl.BlockSpec((h, both * rows), lambda g, i: (0, g)) for h in heights],
            scratch_shapes=[
                pltpu.VMEM((cap, lanes), jnp.float32),
                pltpu.VMEM((both, HEAD_DIM + META, lanes), jnp.float32),
            ],
        ),
        out_shape=[
            jax.ShapeDtypeStruct((h, forks * rows), jnp.int16 if c else jnp.float32)
            for h, c in zip(heights, codes)
        ],
        compiler_params=pltpu.CompilerParams(vmem_limit_bytes=8 * 2**20),
        cost_estimate=pl.CostEstimate(
            flops=4 * forks * lanes * keys * HEAD_DIM,
            transcendentals=forks * lanes * keys,
            bytes_accessed=2 * forks * keys * width,
        ),
        name="parts",
    )(info, *blocks_q, fresh, cache)


def merge_kernel(*refs):
    n = len(refs) // 3
    for k in range(n):
        msg, part, out = refs[2 * k], refs[2 * k + 1], refs[2 * n + k]
        for at in range(0, msg.shape[1], 128):
            sl = slice(at, at + 128)
            top, total, numer = joined([sent_part(msg, sl), held_part(part, sl)])
            code_part(top, total, numer, out, sl)


def merge(*pairs):
    return pl.pallas_call(
        merge_kernel,
        out_shape=[jax.ShapeDtypeStruct(pairs[2 * k].shape, jnp.int16) for k in range(len(pairs) // 2)],
        compiler_params=pltpu.CompilerParams(vmem_limit_bytes=8 * 2**20),
        name="merge",
    )(*pairs)


def finish_kernel(tokens, rows, info, span, own, right, left, out):
    me = info[0]
    forks = own.shape[1] // rows
    both = 128 // rows
    spot = lax.rem(lax.broadcasted_iota(jnp.int32, (rows, HEAD_DIM), 0), tokens) + me * tokens
    for g in range(forks // both):
        sl = slice(g * 128, (g + 1) * 128)
        _, total, numer = joined([held_part(own, sl), sent_part(right, sl), sent_part(left, sl)])
        turned = (numer / total).T
        for j in range(both):
            f = g * both + j
            value = turned[j * rows : (j + 1) * rows]
            out[f] = jnp.where(spot < span[f], value, 0.0).astype(jnp.bfloat16)


def finish(info, span, own, right, left, tokens, rows):
    forks = own.shape[1] // rows
    smem = pl.BlockSpec(memory_space=pltpu.SMEM)
    vmem = pl.BlockSpec(memory_space=pltpu.VMEM)
    return pl.pallas_call(
        functools.partial(finish_kernel, tokens, rows),
        in_specs=[smem, smem, vmem, vmem, vmem],
        out_specs=vmem,
        out_shape=jax.ShapeDtypeStruct((forks, rows, HEAD_DIM), jnp.bfloat16),
        compiler_params=pltpu.CompilerParams(vmem_limit_bytes=8 * 2**20),
        name="finish",
    )(info, span, own, right, left)


def own_kernel(offsets, tokens, info, span, owner, *refs):
    members = len(offsets)
    out = refs[members]
    me = info[0]
    forks = refs[0].shape[0]
    row = lax.rem(lax.broadcasted_iota(jnp.int32, (2 * tokens, HEAD_DIM), 0), tokens)
    for off, ref in zip(offsets, refs):
        first = lax.rem(me + (off + members), members) * tokens
        picked = jnp.zeros((2 * tokens, HEAD_DIM), jnp.float32)
        for f in range(forks):
            mine = (owner[f] == me) & (row + first < span[f])
            picked = jnp.where(mine, ref[f].astype(jnp.float32), picked)
        at = pl.ds(pl.multiple_of(first, tokens), tokens)
        out[at, :HEAD_DIM] = picked[:tokens]
        out[at, HEAD_DIM:] = picked[tokens:]


def own_kv(info, span, owner, q, tokens, width):
    offsets = tuple(q)
    forks, carried, _ = q[0].shape
    smem = pl.BlockSpec(memory_space=pltpu.SMEM)
    at = carried // (2 * tokens) - 1
    tokens_all = len(offsets) * tokens
    return pl.pallas_call(
        functools.partial(own_kernel, offsets, tokens),
        grid=(1,),
        in_specs=[smem] * 3
        + [pl.BlockSpec((forks, 2 * tokens, HEAD_DIM), lambda g: (0, at, 0))] * len(offsets),
        out_specs=pl.BlockSpec((tokens_all, width), lambda g: (0, 0)),
        out_shape=jax.ShapeDtypeStruct((tokens_all, width), jnp.float32),
        compiler_params=pltpu.CompilerParams(vmem_limit_bytes=8 * 2**20),
        name="own_kv",
    )(info, span, owner, *[q[o] for o in offsets]).astype(jnp.bfloat16)


def body(queries, tool_key_value, cache, placed, blocks, span_len, owner):
    forks, tokens, width = tool_key_value.shape
    heads = queries.shape[2] // HEAD_DIM
    rows = heads * tokens
    me = lax.axis_index("inst")
    members = lax.axis_size("inst")
    half = members // 2
    live = placed[:, 0] * blocks[:, 0] * BLOCK
    info = jnp.concatenate([me.astype(jnp.int32)[None], live])
    own_q = queries.reshape(forks, tokens, heads, HEAD_DIM).transpose(0, 2, 1, 3)
    own_kv_rows = tool_key_value.reshape(forks, tokens, 2, HEAD_DIM).transpose(0, 2, 1, 3)
    own_q = jnp.concatenate(
        [own_q.reshape(forks, rows, HEAD_DIM), own_kv_rows.reshape(forks, 2 * tokens, HEAD_DIM)], axis=1
    )

    q = {0: own_q}
    for k in range(1, half + 1):
        q[-k] = passed_along(q[1 - k], 1)
        if k < half:
            q[k] = passed_along(q[k - 1], -1)
    part = {}
    for offsets in CALLS(half):
        codes = tuple(o in (-half, half - 1) for o in offsets)
        got = parts_of([q[o] for o in offsets], offsets, codes, info, cache, own_q, members, tokens)
        part.update(zip(offsets, got))

    left, right = part[-half], part[half - 1]
    for k in range(half - 1, 0, -1):
        left = passed_along(left, -1)
        right = passed_along(right, 1)
        if k > 1:
            left, right = merge(left, part[-k], right, part[k - 1])
        else:
            (left,) = merge(left, part[-1])
    left = passed_along(left, -1)
    owned = own_kv(info, span_len, owner, q, tokens, width).reshape(1, 1, members * tokens, width)
    attended = finish(info, span_len, part[0], right, left, tokens, rows)
    attended = attended.reshape(forks, heads, tokens, HEAD_DIM).transpose(0, 2, 1, 3)
    return attended.reshape(forks, tokens, heads * HEAD_DIM), owned


def CALLS(half):
    order = [0]
    for k in range(1, half + 1):
        order += [-k, k] if k < half else [-k]
    calls = [tuple(order[i : i + 4]) for i in range(0, len(order) - 4, 4)]
    return calls + [tuple(order[-4:-1]), tuple(order[-1:])]


def solution(mesh):
    return jax.shard_map(
        body,
        mesh=mesh,
        in_specs=(
            P(("groups", "rep"), "inst", "tp"),
            P(("groups", "rep"), "inst", "tp"),
            P(("groups", "rep"), "inst", "tp"),
            P(("groups", "rep"), "inst"),
            P(("groups", "rep"), "inst"),
            P(("groups", "rep")),
            P(("groups", "rep")),
        ),
        out_specs=(P(("groups", "rep"), "inst", "tp"), P(("groups", "inst"), "rep", None, "tp")),
        check_vma=False,
    )
```

```python
import functools
import math

import jax
import jax.numpy as jnp
from jax import lax
from jax.experimental import pallas as pl
from jax.experimental.pallas import tpu as pltpu
from jax.sharding import PartitionSpec as P

HEAD_DIM = 128
BLOCK = 128
STEP = 256
META = 8
CODE = 16
NEVER = -1e30
WIDE = 4096.0
FLOOR = -2000.0
NT = (((1,), (1,)), ((), ()))
TN = (((0,), (0,)), ((), ()))


def passed_along(x, by):
    size = lax.axis_size("inst")
    return lax.ppermute(x, "inst", [(i, (i + by) % size) for i in range(size)])


def meta_rows(rows, one, two, three):
    row = lax.broadcasted_iota(jnp.int32, (rows, one.shape[1]), 0)
    return jnp.where(row == 0, one, jnp.where(row == 1, two, three))


def whole(x):
    return jnp.floor(x + 0.5)


def coded(level, mean, out, sl):
    power = jnp.ceil(jnp.log2(jnp.maximum(jnp.max(jnp.abs(mean), axis=0, keepdims=True), 1e-30)))
    steps = whole(mean * jnp.exp2(15.0 - power))
    out[:HEAD_DIM, sl] = jnp.clip(steps, -32767.0, 32767.0).astype(jnp.int32).astype(jnp.int16)
    eighths = whole(level * 8.0)
    rest = whole((level - eighths * 0.125) * 2.0**18)
    out[HEAD_DIM:, sl] = meta_rows(CODE, eighths, rest, power).astype(jnp.int32).astype(jnp.int16)


def code_part(top, total, numer, out, sl):
    held = jnp.maximum(total, 1e-30)
    coded(jnp.maximum(top + jnp.log2(held), FLOOR), numer * (1.0 / held), out, sl)


def decoded(msg, sl):
    x = msg[:, sl].astype(jnp.int32).astype(jnp.float32)
    level = x[HEAD_DIM : HEAD_DIM + 1] * 0.125 + x[HEAD_DIM + 1 : HEAD_DIM + 2] * 2.0**-18
    return level, x[:HEAD_DIM] * jnp.exp2(x[HEAD_DIM + 2 : HEAD_DIM + 3] - 15.0)


def joined(parts):
    top = functools.reduce(jnp.maximum, [p[0] for p in parts])
    total, numer = 0.0, 0.0
    for t, l, n in parts:
        by = jnp.exp2(t - top)
        total = total + by * l
        numer = numer + by * n
    return top, total, numer


def held_part(ref, sl):
    return ref[HEAD_DIM : HEAD_DIM + 1, sl], ref[HEAD_DIM + 1 : HEAD_DIM + 2, sl], ref[:HEAD_DIM, sl]


def sent_part(msg, sl):
    level, mean = decoded(msg, sl)
    return level, 1.0, mean


def part_kernel(offsets, codes, members, tokens, rows, info, *refs):
    n = len(offsets)
    q_refs, fresh_ref, kv_ref = refs[:n], refs[n], refs[n + 1]
    out_refs, s_ref, o_ref = refs[n + 2 : 2 * n + 2], refs[2 * n + 2], refs[2 * n + 3]
    forks = kv_ref.shape[0]
    cap = kv_ref.shape[1]
    lanes = n * rows
    g = pl.program_id(0)
    me = info[0]
    unit = math.log2(math.e) / math.sqrt(HEAD_DIM)

    lane = lax.broadcasted_iota(jnp.int32, (1, lanes), 1)
    first = jnp.zeros((1, lanes), jnp.int32)
    for b, off in enumerate(offsets):
        here = lax.rem(me + (off + members), members) * tokens
        first = jnp.where((lane >= b * rows) & (lane < (b + 1) * rows), here, first)
    q_token = first + lax.rem(lane, tokens)
    u = lax.broadcasted_iota(jnp.int32, (2 * tokens, lanes), 0)
    seen = (u < tokens) & (me * tokens + u <= q_token)

    def one(j, steps):
        q = jnp.concatenate([r[j] for r in q_refs], axis=0)
        fresh = fresh_ref[j]
        live = info[1 + g * forks + j]
        s_new = lax.dot_general(fresh, q, NT, preferred_element_type=jnp.float32)
        s_new = jnp.where(seen, s_new, -jnp.inf)
        top = jnp.max(s_new, axis=0, keepdims=True)
        for c in range(steps):
            at = c * STEP
            s = lax.dot_general(
                kv_ref[j, at : at + STEP, :HEAD_DIM], q, NT, preferred_element_type=jnp.float32
            )
            if c == steps - 1:
                tail = jnp.where(at + BLOCK < live, s[BLOCK:], -jnp.inf)
                s_ref[at : at + BLOCK] = s[:BLOCK]
                s_ref[at + BLOCK : at + STEP] = tail
                top = jnp.maximum(top, jnp.max(s[:BLOCK], axis=0, keepdims=True))
                top = jnp.maximum(top, jnp.max(tail, axis=0, keepdims=True))
            else:
                s_ref[at : at + STEP] = s
                top = jnp.maximum(top, jnp.max(s, axis=0, keepdims=True))
        top = jnp.maximum(top, NEVER)
        w = jnp.exp2((s_new - top) * unit)
        total = jnp.sum(w, axis=0, keepdims=True)
        w = jnp.concatenate([w[tokens:], w[:tokens]], axis=0)
        numer = lax.dot_general(fresh, w.astype(jnp.bfloat16), TN, preferred_element_type=jnp.float32)
        for c in range(steps):
            at = c * STEP
            w = jnp.exp2((s_ref[at : at + STEP] - top) * unit)
            total = total + jnp.sum(w, axis=0, keepdims=True)
            numer = numer + lax.dot_general(
                kv_ref[j, at : at + STEP, HEAD_DIM:],
                w.astype(jnp.bfloat16),
                TN,
                preferred_element_type=jnp.float32,
            )
        o_ref[j, :HEAD_DIM] = numer
        row = lax.broadcasted_iota(jnp.int32, (META, lanes), 0)
        o_ref[j, HEAD_DIM:] = jnp.where(row == 0, top * unit, total)

    def fork(j, carry):
        live = info[1 + g * forks + j]
        for steps in range(cap // STEP + 1):
            pl.when((live > (steps - 1) * STEP) & (live <= steps * STEP))(
                functools.partial(one, j, steps)
            )
        return carry

    lax.fori_loop(0, forks, fork, 0)
    for b in range(n):
        o = jnp.concatenate([o_ref[j, :, b * rows : (b + 1) * rows] for j in range(forks)], axis=1)
        if codes[b]:
            code_part(o[HEAD_DIM : HEAD_DIM + 1], o[HEAD_DIM + 1 : HEAD_DIM + 2], o[:HEAD_DIM], out_refs[b], slice(None))
        else:
            out_refs[b][...] = o


def parts_of(blocks_q, offsets, codes, info, cache, fresh, tokens):
    n = len(offsets)
    members, forks, carried, _ = blocks_q.shape
    rows = carried - 2 * tokens
    both = 128 // rows
    cap, width = cache.shape[1:]
    keys = cap + tokens
    lanes = n * rows
    heights = [HEAD_DIM + (CODE if c else META) for c in codes]
    return pl.pallas_call(
        functools.partial(part_kernel, offsets, codes, members, tokens, rows),
        grid_spec=pltpu.PrefetchScalarGridSpec(
            num_scalar_prefetch=1,
            grid=(forks // both,),
            in_specs=[
                pl.BlockSpec(
                    (None, both, rows, HEAD_DIM),
                    lambda g, i, off=off: (lax.rem(i[0] + (off + members), members), g, 0, 0),
                )
                for off in offsets
            ]
            + [
                pl.BlockSpec((both, 2 * tokens, HEAD_DIM), lambda g, i: (g, 0, 0)),
                pl.BlockSpec((both, cap, width), lambda g, i: (g, 0, 0)),
            ],
            out_specs=[pl.BlockSpec((h, both * rows), lambda g, i: (0, g)) for h in heights],
            scratch_shapes=[
                pltpu.VMEM((cap, lanes), jnp.float32),
                pltpu.VMEM((both, HEAD_DIM + META, lanes), jnp.float32),
            ],
        ),
        out_shape=[
            jax.ShapeDtypeStruct((h, forks * rows), jnp.int16 if c else jnp.float32)
            for h, c in zip(heights, codes)
        ],
        compiler_params=pltpu.CompilerParams(vmem_limit_bytes=8 * 2**20),
        cost_estimate=pl.CostEstimate(
            flops=4 * forks * lanes * keys * HEAD_DIM,
            transcendentals=forks * lanes * keys,
            bytes_accessed=2 * forks * keys * width,
        ),
        name="parts",
    )(info, *[blocks_q] * n, fresh, cache)


def merge_kernel(*refs):
    n = len(refs) // 3
    for k in range(n):
        msg, part, out = refs[2 * k], refs[2 * k + 1], refs[2 * n + k]
        for at in range(0, msg.shape[1], 128):
            sl = slice(at, at + 128)
            top, total, numer = joined([sent_part(msg, sl), held_part(part, sl)])
            code_part(top, total, numer, out, sl)


def merge(*pairs):
    return pl.pallas_call(
        merge_kernel,
        out_shape=[jax.ShapeDtypeStruct(pairs[2 * k].shape, jnp.int16) for k in range(len(pairs) // 2)],
        compiler_params=pltpu.CompilerParams(vmem_limit_bytes=8 * 2**20),
        name="merge",
    )(*pairs)


def finish_kernel(tokens, rows, info, span, own, right, left, out):
    me = info[0]
    forks = own.shape[1] // rows
    both = 128 // rows
    spot = lax.rem(lax.broadcasted_iota(jnp.int32, (rows, HEAD_DIM), 0), tokens) + me * tokens
    for g in range(forks // both):
        sl = slice(g * 128, (g + 1) * 128)
        _, total, numer = joined([held_part(own, sl), sent_part(right, sl), sent_part(left, sl)])
        turned = (numer / total).T
        for j in range(both):
            f = g * both + j
            value = turned[j * rows : (j + 1) * rows]
            out[f] = jnp.where(spot < span[f], value, 0.0).astype(jnp.bfloat16)


def finish(info, span, own, right, left, tokens, rows):
    forks = own.shape[1] // rows
    smem = pl.BlockSpec(memory_space=pltpu.SMEM)
    vmem = pl.BlockSpec(memory_space=pltpu.VMEM)
    return pl.pallas_call(
        functools.partial(finish_kernel, tokens, rows),
        in_specs=[smem, smem, vmem, vmem, vmem],
        out_specs=vmem,
        out_shape=jax.ShapeDtypeStruct((forks, rows, HEAD_DIM), jnp.bfloat16),
        compiler_params=pltpu.CompilerParams(vmem_limit_bytes=8 * 2**20),
        name="finish",
    )(info, span, own, right, left)


def own_kernel(tokens, info, span, owner, rows_ref, out):
    members, forks = rows_ref.shape[:2]
    me = info[0]
    row = lax.rem(lax.broadcasted_iota(jnp.int32, (2 * tokens, HEAD_DIM), 0), tokens)
    for i in range(members):
        picked = jnp.zeros((2 * tokens, HEAD_DIM), jnp.float32)
        for f in range(forks):
            mine = (owner[f] == me) & (row + i * tokens < span[f])
            picked = jnp.where(mine, rows_ref[i, f].astype(jnp.float32), picked)
        out[i * tokens : (i + 1) * tokens, :HEAD_DIM] = picked[:tokens]
        out[i * tokens : (i + 1) * tokens, HEAD_DIM:] = picked[tokens:]


def own_kv(info, span, owner, q, tokens, width):
    members, forks, carried, _ = q.shape
    smem = pl.BlockSpec(memory_space=pltpu.SMEM)
    at = carried // (2 * tokens) - 1
    return pl.pallas_call(
        functools.partial(own_kernel, tokens),
        grid=(1,),
        in_specs=[smem] * 3
        + [pl.BlockSpec((members, forks, 2 * tokens, HEAD_DIM), lambda g: (0, 0, at, 0))],
        out_specs=pl.BlockSpec((members * tokens, width), lambda g: (0, 0)),
        out_shape=jax.ShapeDtypeStruct((members * tokens, width), jnp.float32),
        compiler_params=pltpu.CompilerParams(vmem_limit_bytes=8 * 2**20),
        name="own_kv",
    )(info, span, owner, q).astype(jnp.bfloat16)


def body(queries, tool_key_value, cache, placed, blocks, span_len, owner):
    forks, tokens, width = tool_key_value.shape
    heads = queries.shape[2] // HEAD_DIM
    rows = heads * tokens
    me = lax.axis_index("inst")
    members = lax.axis_size("inst")
    half = members // 2
    live = placed[:, 0] * blocks[:, 0] * BLOCK
    info = jnp.concatenate([me.astype(jnp.int32)[None], live])
    own_q = queries.reshape(forks, tokens, heads, HEAD_DIM).transpose(0, 2, 1, 3)
    fresh = tool_key_value.reshape(forks, tokens, 2, HEAD_DIM).transpose(0, 2, 1, 3)
    own_q, fresh = own_q.reshape(forks, rows, HEAD_DIM), fresh.reshape(forks, 2 * tokens, HEAD_DIM)
    sent = jnp.concatenate([own_q, fresh], axis=1).astype(jnp.float32) * WIDE
    q = lax.all_gather(sent.astype(jnp.float16), "inst", axis=0)
    q = (q.astype(jnp.float32) * (1.0 / WIDE)).astype(jnp.bfloat16)

    part = {}
    for offsets in CALLS(half):
        codes = tuple(o in (-half, half - 1) for o in offsets)
        got = parts_of(q, offsets, codes, info, cache, fresh, tokens)
        part.update(zip(offsets, got))

    left, right = part[-half], part[half - 1]
    for k in range(half - 1, 0, -1):
        left = passed_along(left, -1)
        right = passed_along(right, 1)
        (left,) = merge(left, part[-k])
        if k > 1:
            (right,) = merge(right, part[k - 1])
    left = passed_along(left, -1)
    owned = own_kv(info, span_len, owner, q, tokens, width).reshape(1, 1, members * tokens, width)
    attended = finish(info, span_len, part[0], right, left, tokens, rows)
    attended = attended.reshape(forks, heads, tokens, HEAD_DIM).transpose(0, 2, 1, 3)
    return attended.reshape(forks, tokens, heads * HEAD_DIM), owned


def CALLS(half):
    order = []
    for k in range(half, 0, -1):
        order += [-k, k - 1]
    return [tuple(order[:2])] + [tuple(order[i : i + 4]) for i in range(2, len(order), 4)]


def solution(mesh):
    return jax.shard_map(
        body,
        mesh=mesh,
        in_specs=(
            P(("groups", "rep"), "inst", "tp"),
            P(("groups", "rep"), "inst", "tp"),
            P(("groups", "rep"), "inst", "tp"),
            P(("groups", "rep"), "inst"),
            P(("groups", "rep"), "inst"),
            P(("groups", "rep")),
            P(("groups", "rep")),
        ),
        out_specs=(P(("groups", "rep"), "inst", "tp"), P(("groups", "inst"), "rep", None, "tp")),
        check_vma=False,
    )
```

```python
import functools
import math

import jax
import jax.numpy as jnp
from jax import lax
from jax.experimental import pallas as pl
from jax.experimental.pallas import tpu as pltpu
from jax.sharding import PartitionSpec as P

HEAD_DIM = 128
BLOCK = 128
STEP = 256
META = 8
CODE = 8
NEVER = -1e30
WIDE = 4096.0
FLOOR = -2000.0
NT = (((1,), (1,)), ((), ()))
TN = (((0,), (0,)), ((), ()))


def passed_along(x, by):
    size = lax.axis_size("inst")
    return lax.ppermute(x, "inst", [(i, (i + by) % size) for i in range(size)])


def meta_rows(rows, one, two, three):
    row = lax.broadcasted_iota(jnp.int32, (rows, one.shape[1]), 0)
    return jnp.where(row == 0, one, jnp.where(row == 1, two, three))


def whole(x):
    return jnp.floor(x + 0.5)


def coded(level, mean, out, sl):
    power = jnp.ceil(jnp.log2(jnp.maximum(jnp.max(jnp.abs(mean), axis=0, keepdims=True), 1e-30)))
    steps = whole(mean * jnp.exp2(15.0 - power))
    out[:HEAD_DIM, sl] = jnp.clip(steps, -32767.0, 32767.0).astype(jnp.int32).astype(jnp.int16)
    eighths = whole(level * 8.0)
    rest = whole((level - eighths * 0.125) * 2.0**18)
    out[HEAD_DIM:, sl] = meta_rows(CODE, eighths, rest, power).astype(jnp.int32).astype(jnp.int16)


def code_part(top, total, numer, out, sl):
    held = jnp.maximum(total, 1e-30)
    coded(jnp.maximum(top + jnp.log2(held), FLOOR), numer * (1.0 / held), out, sl)


def decoded(msg, sl):
    x = msg[:, sl].astype(jnp.int32).astype(jnp.float32)
    level = x[HEAD_DIM : HEAD_DIM + 1] * 0.125 + x[HEAD_DIM + 1 : HEAD_DIM + 2] * 2.0**-18
    return level, x[:HEAD_DIM] * jnp.exp2(x[HEAD_DIM + 2 : HEAD_DIM + 3] - 15.0)


def joined(parts):
    top = functools.reduce(jnp.maximum, [p[0] for p in parts])
    total, numer = 0.0, 0.0
    for t, l, n in parts:
        by = jnp.exp2(t - top)
        total = total + by * l
        numer = numer + by * n
    return top, total, numer


def held_part(ref, sl):
    return ref[HEAD_DIM : HEAD_DIM + 1, sl], ref[HEAD_DIM + 1 : HEAD_DIM + 2, sl], ref[:HEAD_DIM, sl]


def sent_part(msg, sl):
    level, mean = decoded(msg, sl)
    return level, 1.0, mean


def part_kernel(offset, code, tokens, info, q_ref, fresh_ref, kv_ref, *rest):
    out, s_ref = rest[-2:]
    members, forks, carried, _ = q_ref.shape
    rows = carried - 2 * tokens
    both = 128 // rows
    cap = kv_ref.shape[1]
    me = info[0]
    unit = math.log2(math.e) / math.sqrt(HEAD_DIM)

    lane = lax.broadcasted_iota(jnp.int32, (1, 128), 1)
    place = lane // rows
    block = lax.rem(me + (offset + members), members)
    u = lax.broadcasted_iota(jnp.int32, (2 * tokens, 128), 0)
    seen = (u < tokens) & (me * tokens + u <= block * tokens + lax.rem(lane, tokens))
    empty = jnp.zeros((rows, HEAD_DIM), jnp.bfloat16)

    def several(g, steps):
        fork = [g * both + j for j in range(both)]
        live = jnp.full((1, 128), info[1 + fork[0]], jnp.int32)
        for j in range(1, both):
            live = jnp.where(place == j, info[1 + fork[j]], live)
        q = jnp.concatenate(
            [
                jnp.concatenate([q_ref[block, f, :rows] if k == j else empty for k in range(both)], axis=1)
                for j, f in enumerate(fork)
            ],
            axis=0,
        )
        fresh = jnp.concatenate([fresh_ref[f] for f in fork], axis=1)
        s = lax.dot_general(fresh, q, NT, preferred_element_type=jnp.float32)
        new = jnp.where(seen, s, -jnp.inf)
        top = jnp.max(new, axis=0, keepdims=True)
        for c in range(steps):
            at = c * STEP
            keys = jnp.concatenate([kv_ref[f, at : at + STEP, :HEAD_DIM] for f in fork], axis=1)
            s = lax.dot_general(keys, q, NT, preferred_element_type=jnp.float32)
            for lo in range(0, STEP, BLOCK):
                part = jnp.where(at + lo < live, s[lo : lo + BLOCK], -jnp.inf)
                s_ref[at + lo : at + lo + BLOCK] = part
                top = jnp.maximum(top, jnp.max(part, axis=0, keepdims=True))
        top = jnp.maximum(top, NEVER)
        w = jnp.exp2((new - top) * unit)
        total = jnp.sum(w, axis=0, keepdims=True)
        w = jnp.concatenate([w[tokens:], w[:tokens]], axis=0).astype(jnp.bfloat16)
        numer = lax.dot_general(fresh, w, TN, preferred_element_type=jnp.float32)
        for c in range(steps):
            at = c * STEP
            w = jnp.exp2((s_ref[at : at + STEP] - top) * unit)
            total = total + jnp.sum(w, axis=0, keepdims=True)
            values = jnp.concatenate([kv_ref[f, at : at + STEP, HEAD_DIM:] for f in fork], axis=1)
            numer = numer + lax.dot_general(
                values, w.astype(jnp.bfloat16), TN, preferred_element_type=jnp.float32
            )
        own = numer[:HEAD_DIM]
        for j in range(1, both):
            own = jnp.where(place == j, numer[j * HEAD_DIM : (j + 1) * HEAD_DIM], own)
        here = pl.ds(pl.multiple_of(g * 128, 128), 128)
        if code:
            code_part(top * unit, total, own, out, here)
        else:
            out[:HEAD_DIM, here] = own
            out[HEAD_DIM:, here] = meta_rows(META, top * unit, total, total)

    def group(g, carry):
        most = functools.reduce(jnp.maximum, [info[1 + g * both + j] for j in range(both)])
        for steps in range(cap // STEP + 1):
            pl.when((most > (steps - 1) * STEP) & (most <= steps * STEP))(
                functools.partial(several, g, steps)
            )
        return carry

    lax.fori_loop(0, forks // both, group, 0)


def part_of(blocks_q, info, cache, fresh, tokens, offset, *after, code=False):
    members, forks, carried, _ = blocks_q.shape
    rows = carried - 2 * tokens
    cap, width = cache.shape[1:]
    keys = cap + tokens
    height = HEAD_DIM + (CODE if code else META)
    vmem = pl.BlockSpec(memory_space=pltpu.VMEM)
    return pl.pallas_call(
        functools.partial(part_kernel, offset, code, tokens),
        in_specs=[pl.BlockSpec(memory_space=pltpu.SMEM)] + [vmem] * (3 + len(after)),
        out_specs=vmem,
        scratch_shapes=[pltpu.VMEM((cap, 128), jnp.float32)],
        out_shape=jax.ShapeDtypeStruct((height, forks * rows), jnp.int16 if code else jnp.float32),
        compiler_params=pltpu.CompilerParams(vmem_limit_bytes=16 * 2**20),
        cost_estimate=pl.CostEstimate(
            flops=4 * forks * rows * keys * HEAD_DIM,
            transcendentals=forks * rows * keys,
            bytes_accessed=2 * forks * keys * width,
        ),
        name="part",
    )(info, blocks_q, fresh, cache, *after)


def merge_kernel(msg, part, out):
    for at in range(0, msg.shape[1], 128):
        sl = slice(at, at + 128)
        top, total, numer = joined([sent_part(msg, sl), held_part(part, sl)])
        code_part(top, total, numer, out, sl)


def merge(msg, part):
    return pl.pallas_call(
        merge_kernel,
        out_shape=jax.ShapeDtypeStruct(msg.shape, msg.dtype),
        compiler_params=pltpu.CompilerParams(vmem_limit_bytes=8 * 2**20),
        name="merge",
    )(msg, part)


def finish_kernel(tokens, rows, info, span, own, right, left, out):
    me = info[0]
    forks = own.shape[1] // rows
    both = 128 // rows
    spot = lax.rem(lax.broadcasted_iota(jnp.int32, (rows, HEAD_DIM), 0), tokens) + me * tokens
    for g in range(forks // both):
        sl = slice(g * 128, (g + 1) * 128)
        _, total, numer = joined([held_part(own, sl), sent_part(right, sl), sent_part(left, sl)])
        turned = (numer / total).T
        for j in range(both):
            f = g * both + j
            value = turned[j * rows : (j + 1) * rows]
            out[f] = jnp.where(spot < span[f], value, 0.0).astype(jnp.bfloat16)


def finish(info, span, own, right, left, tokens, rows):
    forks = own.shape[1] // rows
    smem = pl.BlockSpec(memory_space=pltpu.SMEM)
    vmem = pl.BlockSpec(memory_space=pltpu.VMEM)
    return pl.pallas_call(
        functools.partial(finish_kernel, tokens, rows),
        in_specs=[smem, smem, vmem, vmem, vmem],
        out_specs=vmem,
        out_shape=jax.ShapeDtypeStruct((forks, rows, HEAD_DIM), jnp.bfloat16),
        compiler_params=pltpu.CompilerParams(vmem_limit_bytes=8 * 2**20),
        name="finish",
    )(info, span, own, right, left)


def own_kernel(tokens, info, span, owner, rows_ref, out):
    members, forks = rows_ref.shape[:2]
    me = info[0]
    row = lax.rem(lax.broadcasted_iota(jnp.int32, (2 * tokens, HEAD_DIM), 0), tokens)
    for i in range(members):
        picked = jnp.zeros((2 * tokens, HEAD_DIM), jnp.float32)
        for f in range(forks):
            mine = (owner[f] == me) & (row + i * tokens < span[f])
            picked = jnp.where(mine, rows_ref[i, f].astype(jnp.float32), picked)
        out[i * tokens : (i + 1) * tokens, :HEAD_DIM] = picked[:tokens]
        out[i * tokens : (i + 1) * tokens, HEAD_DIM:] = picked[tokens:]


def own_kv(info, span, owner, q, tokens, width):
    members, forks, carried, _ = q.shape
    smem = pl.BlockSpec(memory_space=pltpu.SMEM)
    at = carried // (2 * tokens) - 1
    return pl.pallas_call(
        functools.partial(own_kernel, tokens),
        grid=(1,),
        in_specs=[smem] * 3
        + [pl.BlockSpec((members, forks, 2 * tokens, HEAD_DIM), lambda g: (0, 0, at, 0))],
        out_specs=pl.BlockSpec((members * tokens, width), lambda g: (0, 0)),
        out_shape=jax.ShapeDtypeStruct((members * tokens, width), jnp.float32),
        compiler_params=pltpu.CompilerParams(vmem_limit_bytes=8 * 2**20),
        name="own_kv",
    )(info, span, owner, q).astype(jnp.bfloat16)


def body(queries, tool_key_value, cache, placed, blocks, span_len, owner):
    forks, tokens, width = tool_key_value.shape
    heads = queries.shape[2] // HEAD_DIM
    rows = heads * tokens
    me = lax.axis_index("inst")
    members = lax.axis_size("inst")
    half = members // 2
    live = placed[:, 0] * blocks[:, 0] * BLOCK
    info = jnp.concatenate([me.astype(jnp.int32)[None], live])
    own_q = queries.reshape(forks, tokens, heads, HEAD_DIM).transpose(0, 2, 1, 3)
    fresh = tool_key_value.reshape(forks, tokens, 2, HEAD_DIM).transpose(0, 2, 1, 3)
    own_q, fresh = own_q.reshape(forks, rows, HEAD_DIM), fresh.reshape(forks, 2 * tokens, HEAD_DIM)
    sent = jnp.concatenate([own_q, fresh], axis=1).astype(jnp.float32) * WIDE
    q = lax.all_gather(sent.astype(jnp.float16), "inst", axis=0)
    q = (q.astype(jnp.float32) * (1.0 / WIDE)).astype(jnp.bfloat16)

    part = functools.partial(part_of, q, info, cache, fresh, tokens)
    right, left = part(half - 1, code=True), part(-half, code=True)
    for k in range(half - 1, 0, -1):
        if k > 1:
            mine = part(k - 1, left)
            right = merge(passed_along(right, 1), mine)
            mine = part(-k, right)
        else:
            right = passed_along(right, 1)
            mine = part(-k, left)
        left = merge(passed_along(left, -1), mine)
    mine = part(0, left)
    left = passed_along(left, -1)
    owned = own_kv(info, span_len, owner, q, tokens, width).reshape(1, 1, members * tokens, width)
    attended = finish(info, span_len, mine, right, left, tokens, rows)
    attended = attended.reshape(forks, heads, tokens, HEAD_DIM).transpose(0, 2, 1, 3)
    return attended.reshape(forks, tokens, heads * HEAD_DIM), owned


def solution(mesh):
    return jax.shard_map(
        body,
        mesh=mesh,
        in_specs=(
            P(("groups", "rep"), "inst", "tp"),
            P(("groups", "rep"), "inst", "tp"),
            P(("groups", "rep"), "inst", "tp"),
            P(("groups", "rep"), "inst"),
            P(("groups", "rep"), "inst"),
            P(("groups", "rep")),
            P(("groups", "rep")),
        ),
        out_specs=(P(("groups", "rep"), "inst", "tp"), P(("groups", "inst"), "rep", None, "tp")),
        check_vma=False,
    )
```

```python
import functools
import math

import jax
import jax.numpy as jnp
from jax import lax
from jax.experimental import pallas as pl
from jax.experimental.pallas import tpu as pltpu
from jax.sharding import PartitionSpec as P

HEAD_DIM = 128
BLOCK = 128
STEP = 256
META = 8
CODE = 8
NEVER = -1e30
WIDE = 4096.0
FLOOR = -2000.0
NT = (((1,), (1,)), ((), ()))
TN = (((0,), (0,)), ((), ()))


def passed_along(x, by):
    size = lax.axis_size("inst")
    return lax.ppermute(x, "inst", [(i, (i + by) % size) for i in range(size)])


def meta_rows(rows, one, two, three):
    row = lax.broadcasted_iota(jnp.int32, (rows, one.shape[1]), 0)
    return jnp.where(row == 0, one, jnp.where(row == 1, two, three))


def whole(x):
    return jnp.floor(x + 0.5)


def coded(level, mean, out, sl):
    power = jnp.ceil(jnp.log2(jnp.maximum(jnp.max(jnp.abs(mean), axis=0, keepdims=True), 1e-30)))
    steps = whole(mean * jnp.exp2(15.0 - power))
    out[:HEAD_DIM, sl] = jnp.clip(steps, -32767.0, 32767.0).astype(jnp.int32).astype(jnp.int16)
    eighths = whole(level * 8.0)
    rest = whole((level - eighths * 0.125) * 2.0**18)
    out[HEAD_DIM:, sl] = meta_rows(CODE, eighths, rest, power).astype(jnp.int32).astype(jnp.int16)


def code_part(top, total, numer, out, sl):
    held = jnp.maximum(total, 1e-30)
    coded(jnp.maximum(top + jnp.log2(held), FLOOR), numer * (1.0 / held), out, sl)


def decoded(msg, sl):
    x = msg[:, sl].astype(jnp.int32).astype(jnp.float32)
    level = x[HEAD_DIM : HEAD_DIM + 1] * 0.125 + x[HEAD_DIM + 1 : HEAD_DIM + 2] * 2.0**-18
    return level, x[:HEAD_DIM] * jnp.exp2(x[HEAD_DIM + 2 : HEAD_DIM + 3] - 15.0)


def joined(parts):
    top = functools.reduce(jnp.maximum, [p[0] for p in parts])
    total, numer = 0.0, 0.0
    for t, l, n in parts:
        by = jnp.exp2(t - top)
        total = total + by * l
        numer = numer + by * n
    return top, total, numer


def held_part(ref, sl):
    return ref[HEAD_DIM : HEAD_DIM + 1, sl], ref[HEAD_DIM + 1 : HEAD_DIM + 2, sl], ref[:HEAD_DIM, sl]


def sent_part(msg, sl):
    level, mean = decoded(msg, sl)
    return level, 1.0, mean


def part_kernel(offsets, codes, tokens, info, q_ref, fresh_ref, kv_ref, *rest):
    n = len(offsets)
    outs, s_ref = rest[:n], rest[n]
    members, forks, carried, _ = q_ref.shape
    rows = carried - 2 * tokens
    both = 128 // rows
    cap = kv_ref.shape[1]
    lanes = n * rows
    me = info[0]
    unit = math.log2(math.e) / math.sqrt(HEAD_DIM)

    lane = lax.broadcasted_iota(jnp.int32, (1, lanes), 1)
    blocks = [lax.rem(me + (off + members), members) for off in offsets]
    first = jnp.zeros((1, lanes), jnp.int32)
    for b, block in enumerate(blocks):
        first = jnp.where((lane >= b * rows) & (lane < (b + 1) * rows), block * tokens, first)
    q_token = first + lax.rem(lane, tokens)
    u = lax.broadcasted_iota(jnp.int32, (2 * tokens, lanes), 0)
    seen = (u < tokens) & (me * tokens + u <= q_token)

    def several(g, steps):
        fork = [g * both + j for j in range(both)]
        live = [info[1 + f] for f in fork]
        q = [jnp.concatenate([q_ref[i, f, :rows] for i in blocks], axis=0) for f in fork]
        fresh = [fresh_ref[f] for f in fork]
        new, top = [], []
        for j in range(both):
            s = lax.dot_general(fresh[j], q[j], NT, preferred_element_type=jnp.float32)
            new.append(jnp.where(seen, s, -jnp.inf))
            top.append(jnp.max(new[j], axis=0, keepdims=True))
        for c in range(steps):
            for j in range(both):
                at = c * STEP
                keys = kv_ref[fork[j], at : at + STEP, :HEAD_DIM]
                s = lax.dot_general(keys, q[j], NT, preferred_element_type=jnp.float32)
                for lo in range(0, STEP, BLOCK):
                    part = jnp.where(at + lo < live[j], s[lo : lo + BLOCK], -jnp.inf)
                    s_ref[j, at + lo : at + lo + BLOCK] = part
                    top[j] = jnp.maximum(top[j], jnp.max(part, axis=0, keepdims=True))
        top = [jnp.maximum(t, NEVER) for t in top]
        total, numer = [], []
        for j in range(both):
            w = jnp.exp2((new[j] - top[j]) * unit)
            total.append(jnp.sum(w, axis=0, keepdims=True))
            w = jnp.concatenate([w[tokens:], w[:tokens]], axis=0).astype(jnp.bfloat16)
            numer.append(lax.dot_general(fresh[j], w, TN, preferred_element_type=jnp.float32))
        for c in range(steps):
            for j in range(both):
                at = c * STEP
                w = jnp.exp2((s_ref[j, at : at + STEP] - top[j]) * unit)
                total[j] = total[j] + jnp.sum(w, axis=0, keepdims=True)
                values = kv_ref[fork[j], at : at + STEP, HEAD_DIM:]
                numer[j] = numer[j] + lax.dot_general(
                    values, w.astype(jnp.bfloat16), TN, preferred_element_type=jnp.float32
                )
        here = pl.ds(pl.multiple_of(g * 128, 128), 128)
        for b in range(n):
            mine = slice(b * rows, (b + 1) * rows)
            t, l, o = (jnp.concatenate([x[:, mine] for x in xs], axis=1) for xs in (top, total, numer))
            if codes[b]:
                code_part(t * unit, l, o, outs[b], here)
            else:
                outs[b][:HEAD_DIM, here] = o
                outs[b][HEAD_DIM:, here] = meta_rows(META, t * unit, l, l)

    def group(g, carry):
        most = functools.reduce(jnp.maximum, [info[1 + g * both + j] for j in range(both)])
        for steps in range(cap // STEP + 1):
            pl.when((most > (steps - 1) * STEP) & (most <= steps * STEP))(
                functools.partial(several, g, steps)
            )
        return carry

    lax.fori_loop(0, forks // both, group, 0)


def parts_of(blocks_q, offsets, codes, info, cache, fresh, tokens):
    n = len(offsets)
    members, forks, carried, _ = blocks_q.shape
    rows = carried - 2 * tokens
    cap, width = cache.shape[1:]
    keys = cap + tokens
    lanes = n * rows
    heights = [HEAD_DIM + (CODE if c else META) for c in codes]
    vmem = pl.BlockSpec(memory_space=pltpu.VMEM)
    return pl.pallas_call(
        functools.partial(part_kernel, offsets, codes, tokens),
        in_specs=[pl.BlockSpec(memory_space=pltpu.SMEM), vmem, vmem, vmem],
        out_specs=[vmem] * n,
        scratch_shapes=[pltpu.VMEM((128 // rows, cap, lanes), jnp.float32)],
        out_shape=[
            jax.ShapeDtypeStruct((h, forks * rows), jnp.int16 if c else jnp.float32)
            for h, c in zip(heights, codes)
        ],
        compiler_params=pltpu.CompilerParams(vmem_limit_bytes=16 * 2**20),
        cost_estimate=pl.CostEstimate(
            flops=4 * forks * lanes * keys * HEAD_DIM,
            transcendentals=forks * lanes * keys,
            bytes_accessed=2 * forks * keys * width,
        ),
        name="parts",
    )(info, blocks_q, fresh, cache)


def merge_kernel(*refs):
    n = len(refs) // 3
    for k in range(n):
        msg, part, out = refs[2 * k], refs[2 * k + 1], refs[2 * n + k]
        for at in range(0, msg.shape[1], 128):
            sl = slice(at, at + 128)
            top, total, numer = joined([sent_part(msg, sl), held_part(part, sl)])
            code_part(top, total, numer, out, sl)


def merge(*pairs):
    return pl.pallas_call(
        merge_kernel,
        out_shape=[jax.ShapeDtypeStruct(pairs[2 * k].shape, jnp.int16) for k in range(len(pairs) // 2)],
        compiler_params=pltpu.CompilerParams(vmem_limit_bytes=8 * 2**20),
        name="merge",
    )(*pairs)


def finish_kernel(tokens, rows, info, span, own, right, left, out):
    me = info[0]
    forks = own.shape[1] // rows
    both = 128 // rows
    spot = lax.rem(lax.broadcasted_iota(jnp.int32, (rows, HEAD_DIM), 0), tokens) + me * tokens
    for g in range(forks // both):
        sl = slice(g * 128, (g + 1) * 128)
        _, total, numer = joined([held_part(own, sl), sent_part(right, sl), sent_part(left, sl)])
        turned = (numer / total).T
        for j in range(both):
            f = g * both + j
            value = turned[j * rows : (j + 1) * rows]
            out[f] = jnp.where(spot < span[f], value, 0.0).astype(jnp.bfloat16)


def finish(info, span, own, right, left, tokens, rows):
    forks = own.shape[1] // rows
    smem = pl.BlockSpec(memory_space=pltpu.SMEM)
    vmem = pl.BlockSpec(memory_space=pltpu.VMEM)
    return pl.pallas_call(
        functools.partial(finish_kernel, tokens, rows),
        in_specs=[smem, smem, vmem, vmem, vmem],
        out_specs=vmem,
        out_shape=jax.ShapeDtypeStruct((forks, rows, HEAD_DIM), jnp.bfloat16),
        compiler_params=pltpu.CompilerParams(vmem_limit_bytes=8 * 2**20),
        name="finish",
    )(info, span, own, right, left)


def own_kernel(tokens, info, span, owner, rows_ref, out):
    members, forks = rows_ref.shape[:2]
    me = info[0]
    row = lax.rem(lax.broadcasted_iota(jnp.int32, (2 * tokens, HEAD_DIM), 0), tokens)
    for i in range(members):
        picked = jnp.zeros((2 * tokens, HEAD_DIM), jnp.float32)
        for f in range(forks):
            mine = (owner[f] == me) & (row + i * tokens < span[f])
            picked = jnp.where(mine, rows_ref[i, f].astype(jnp.float32), picked)
        out[i * tokens : (i + 1) * tokens, :HEAD_DIM] = picked[:tokens]
        out[i * tokens : (i + 1) * tokens, HEAD_DIM:] = picked[tokens:]


def own_kv(info, span, owner, q, tokens, width):
    members, forks, carried, _ = q.shape
    smem = pl.BlockSpec(memory_space=pltpu.SMEM)
    at = carried // (2 * tokens) - 1
    return pl.pallas_call(
        functools.partial(own_kernel, tokens),
        grid=(1,),
        in_specs=[smem] * 3
        + [pl.BlockSpec((members, forks, 2 * tokens, HEAD_DIM), lambda g: (0, 0, at, 0))],
        out_specs=pl.BlockSpec((members * tokens, width), lambda g: (0, 0)),
        out_shape=jax.ShapeDtypeStruct((members * tokens, width), jnp.float32),
        compiler_params=pltpu.CompilerParams(vmem_limit_bytes=8 * 2**20),
        name="own_kv",
    )(info, span, owner, q).astype(jnp.bfloat16)


def body(queries, tool_key_value, cache, placed, blocks, span_len, owner):
    forks, tokens, width = tool_key_value.shape
    heads = queries.shape[2] // HEAD_DIM
    rows = heads * tokens
    me = lax.axis_index("inst")
    members = lax.axis_size("inst")
    half = members // 2
    live = placed[:, 0] * blocks[:, 0] * BLOCK
    info = jnp.concatenate([me.astype(jnp.int32)[None], live])
    own_q = queries.reshape(forks, tokens, heads, HEAD_DIM).transpose(0, 2, 1, 3)
    fresh = tool_key_value.reshape(forks, tokens, 2, HEAD_DIM).transpose(0, 2, 1, 3)
    own_q, fresh = own_q.reshape(forks, rows, HEAD_DIM), fresh.reshape(forks, 2 * tokens, HEAD_DIM)
    sent = jnp.concatenate([own_q, fresh], axis=1).astype(jnp.float32) * WIDE
    q = lax.all_gather(sent.astype(jnp.float16), "inst", axis=0)
    q = (q.astype(jnp.float32) * (1.0 / WIDE)).astype(jnp.bfloat16)

    part = {}
    for offsets in CALLS(half):
        codes = tuple(o in (-half, half - 1) for o in offsets)
        got = parts_of(q, offsets, codes, info, cache, fresh, tokens)
        part.update(zip(offsets, got))

    left, right = part[-half], part[half - 1]
    for k in range(half - 1, 0, -1):
        left = passed_along(left, -1)
        right = passed_along(right, 1)
        (left,) = merge(left, part[-k])
        if k > 1:
            (right,) = merge(right, part[k - 1])
    left = passed_along(left, -1)
    owned = own_kv(info, span_len, owner, q, tokens, width).reshape(1, 1, members * tokens, width)
    attended = finish(info, span_len, part[0], right, left, tokens, rows)
    attended = attended.reshape(forks, heads, tokens, HEAD_DIM).transpose(0, 2, 1, 3)
    return attended.reshape(forks, tokens, heads * HEAD_DIM), owned


def CALLS(half):
    order = []
    for k in range(half, 0, -1):
        order += [-k, k - 1]
    return [tuple(order[:2]), tuple(order[2:])]


def solution(mesh):
    return jax.shard_map(
        body,
        mesh=mesh,
        in_specs=(
            P(("groups", "rep"), "inst", "tp"),
            P(("groups", "rep"), "inst", "tp"),
            P(("groups", "rep"), "inst", "tp"),
            P(("groups", "rep"), "inst"),
            P(("groups", "rep"), "inst"),
            P(("groups", "rep")),
            P(("groups", "rep")),
        ),
        out_specs=(P(("groups", "rep"), "inst", "tp"), P(("groups", "inst"), "rep", None, "tp")),
        check_vma=False,
    )
```

```python
import functools
import math

import jax
import jax.numpy as jnp
from jax import lax
from jax.experimental import pallas as pl
from jax.experimental.pallas import tpu as pltpu
from jax.sharding import PartitionSpec as P

HEAD_DIM = 128
BLOCK = 128
STEP = 256
META = 8
CODE = 8
NEVER = -1e30
WIDE = 4096.0
FLOOR = -2000.0
NT = (((1,), (1,)), ((), ()))
TN = (((0,), (0,)), ((), ()))


def passed_along(x, by):
    size = lax.axis_size("inst")
    return lax.ppermute(x, "inst", [(i, (i + by) % size) for i in range(size)])


def meta_rows(rows, one, two, three):
    row = lax.broadcasted_iota(jnp.int32, (rows, one.shape[1]), 0)
    return jnp.where(row == 0, one, jnp.where(row == 1, two, three))


def whole(x):
    return jnp.floor(x + 0.5)


def coded(level, mean, out, sl):
    power = jnp.ceil(jnp.log2(jnp.maximum(jnp.max(jnp.abs(mean), axis=0, keepdims=True), 1e-30)))
    steps = whole(mean * jnp.exp2(15.0 - power))
    out[:HEAD_DIM, sl] = jnp.clip(steps, -32767.0, 32767.0).astype(jnp.int32).astype(jnp.int16)
    eighths = whole(level * 8.0)
    rest = whole((level - eighths * 0.125) * 2.0**18)
    out[HEAD_DIM:, sl] = meta_rows(CODE, eighths, rest, power).astype(jnp.int32).astype(jnp.int16)


def code_part(top, total, numer, out, sl):
    held = jnp.maximum(total, 1e-30)
    coded(jnp.maximum(top + jnp.log2(held), FLOOR), numer * (1.0 / held), out, sl)


def decoded(msg, sl):
    x = msg[:, sl].astype(jnp.int32).astype(jnp.float32)
    level = x[HEAD_DIM : HEAD_DIM + 1] * 0.125 + x[HEAD_DIM + 1 : HEAD_DIM + 2] * 2.0**-18
    return level, x[:HEAD_DIM] * jnp.exp2(x[HEAD_DIM + 2 : HEAD_DIM + 3] - 15.0)


def joined(parts):
    top = functools.reduce(jnp.maximum, [p[0] for p in parts])
    total, numer = 0.0, 0.0
    for t, l, n in parts:
        by = jnp.exp2(t - top)
        total = total + by * l
        numer = numer + by * n
    return top, total, numer


def held_part(ref, sl):
    return ref[HEAD_DIM : HEAD_DIM + 1, sl], ref[HEAD_DIM + 1 : HEAD_DIM + 2, sl], ref[:HEAD_DIM, sl]


def sent_part(msg, sl):
    level, mean = decoded(msg, sl)
    return level, 1.0, mean


def part_kernel(offsets, codes, tokens, info, q_ref, fresh_ref, kv_ref, *rest):
    n = len(offsets)
    outs, s_ref = rest[:n], rest[n]
    members, forks, carried, _ = q_ref.shape
    rows = carried - 2 * tokens
    both = 128 // rows
    cap = kv_ref.shape[1]
    lanes = n * rows
    me = info[0]
    unit = math.log2(math.e) / math.sqrt(HEAD_DIM)

    lane = lax.broadcasted_iota(jnp.int32, (1, lanes), 1)
    blocks = [lax.rem(me + (off + members), members) for off in offsets]
    first = jnp.zeros((1, lanes), jnp.int32)
    for b, block in enumerate(blocks):
        first = jnp.where((lane >= b * rows) & (lane < (b + 1) * rows), block * tokens, first)
    q_token = first + lax.rem(lane, tokens)
    u = lax.broadcasted_iota(jnp.int32, (2 * tokens, lanes), 0)
    seen = (u < tokens) & (me * tokens + u <= q_token)

    def several(g, steps):
        fork = [g * both + j for j in range(both)]
        live = [info[1 + f] for f in fork]
        q = [jnp.concatenate([q_ref[i, f, :rows] for i in blocks], axis=0) for f in fork]
        fresh = [fresh_ref[f] for f in fork]
        new, top = [], []
        for j in range(both):
            s = lax.dot_general(fresh[j], q[j], NT, preferred_element_type=jnp.float32)
            new.append(jnp.where(seen, s, -jnp.inf))
            top.append(jnp.max(new[j], axis=0, keepdims=True))
        for c in range(steps):
            for j in range(both):
                at = c * STEP
                keys = kv_ref[fork[j], at : at + STEP, :HEAD_DIM]
                s = lax.dot_general(keys, q[j], NT, preferred_element_type=jnp.float32)
                for lo in range(0, STEP, BLOCK):
                    part = jnp.where(at + lo < live[j], s[lo : lo + BLOCK], -jnp.inf)
                    s_ref[j, at + lo : at + lo + BLOCK] = part
                    top[j] = jnp.maximum(top[j], jnp.max(part, axis=0, keepdims=True))
        top = [jnp.maximum(t, NEVER) for t in top]
        total, numer = [], []
        for j in range(both):
            w = jnp.exp2((new[j] - top[j]) * unit)
            total.append(jnp.sum(w, axis=0, keepdims=True))
            w = jnp.concatenate([w[tokens:], w[:tokens]], axis=0).astype(jnp.bfloat16)
            numer.append(lax.dot_general(fresh[j], w, TN, preferred_element_type=jnp.float32))
        for c in range(steps):
            for j in range(both):
                at = c * STEP
                w = jnp.exp2((s_ref[j, at : at + STEP] - top[j]) * unit)
                total[j] = total[j] + jnp.sum(w, axis=0, keepdims=True)
                values = kv_ref[fork[j], at : at + STEP, HEAD_DIM:]
                numer[j] = numer[j] + lax.dot_general(
                    values, w.astype(jnp.bfloat16), TN, preferred_element_type=jnp.float32
                )
        here = pl.ds(pl.multiple_of(g * 128, 128), 128)
        for b in range(n):
            mine = slice(b * rows, (b + 1) * rows)
            t, l, o = (jnp.concatenate([x[:, mine] for x in xs], axis=1) for xs in (top, total, numer))
            if codes[b]:
                code_part(t * unit, l, o, outs[b], here)
            else:
                outs[b][:HEAD_DIM, here] = o
                outs[b][HEAD_DIM:, here] = meta_rows(META, t * unit, l, l)

    def group(g, carry):
        most = functools.reduce(jnp.maximum, [info[1 + g * both + j] for j in range(both)])
        for steps in range(cap // STEP + 1):
            pl.when((most > (steps - 1) * STEP) & (most <= steps * STEP))(
                functools.partial(several, g, steps)
            )
        return carry

    lax.fori_loop(0, forks // both, group, 0)


def parts_of(blocks_q, offsets, codes, info, cache, fresh, tokens):
    n = len(offsets)
    members, forks, carried, _ = blocks_q.shape
    rows = carried - 2 * tokens
    cap, width = cache.shape[1:]
    keys = cap + tokens
    lanes = n * rows
    heights = [HEAD_DIM + (CODE if c else META) for c in codes]
    vmem = pl.BlockSpec(memory_space=pltpu.VMEM)
    return pl.pallas_call(
        functools.partial(part_kernel, offsets, codes, tokens),
        in_specs=[pl.BlockSpec(memory_space=pltpu.SMEM), vmem, vmem, vmem],
        out_specs=[vmem] * n,
        scratch_shapes=[pltpu.VMEM((128 // rows, cap, lanes), jnp.float32)],
        out_shape=[
            jax.ShapeDtypeStruct((h, forks * rows), jnp.int16 if c else jnp.float32)
            for h, c in zip(heights, codes)
        ],
        compiler_params=pltpu.CompilerParams(vmem_limit_bytes=16 * 2**20),
        cost_estimate=pl.CostEstimate(
            flops=4 * forks * lanes * keys * HEAD_DIM,
            transcendentals=forks * lanes * keys,
            bytes_accessed=2 * forks * keys * width,
        ),
        name="parts",
    )(info, blocks_q, fresh, cache)


def merge_kernel(*refs):
    n = len(refs) // 3
    for k in range(n):
        msg, part, out = refs[2 * k], refs[2 * k + 1], refs[2 * n + k]
        for at in range(0, msg.shape[1], 128):
            sl = slice(at, at + 128)
            top, total, numer = joined([sent_part(msg, sl), held_part(part, sl)])
            code_part(top, total, numer, out, sl)


def merge(*pairs):
    return pl.pallas_call(
        merge_kernel,
        out_shape=[jax.ShapeDtypeStruct(pairs[2 * k].shape, jnp.int16) for k in range(len(pairs) // 2)],
        compiler_params=pltpu.CompilerParams(vmem_limit_bytes=8 * 2**20),
        name="merge",
    )(*pairs)


def finish_kernel(tokens, rows, info, span, own, right, left, out):
    me = info[0]
    forks = own.shape[1] // rows
    both = 128 // rows
    spot = lax.rem(lax.broadcasted_iota(jnp.int32, (rows, HEAD_DIM), 0), tokens) + me * tokens
    for g in range(forks // both):
        sl = slice(g * 128, (g + 1) * 128)
        _, total, numer = joined([held_part(own, sl), sent_part(right, sl), sent_part(left, sl)])
        turned = (numer / total).T
        for j in range(both):
            f = g * both + j
            value = turned[j * rows : (j + 1) * rows]
            out[f] = jnp.where(spot < span[f], value, 0.0).astype(jnp.bfloat16)


def finish(info, span, own, right, left, tokens, rows):
    forks = own.shape[1] // rows
    smem = pl.BlockSpec(memory_space=pltpu.SMEM)
    vmem = pl.BlockSpec(memory_space=pltpu.VMEM)
    return pl.pallas_call(
        functools.partial(finish_kernel, tokens, rows),
        in_specs=[smem, smem, vmem, vmem, vmem],
        out_specs=vmem,
        out_shape=jax.ShapeDtypeStruct((forks, rows, HEAD_DIM), jnp.bfloat16),
        compiler_params=pltpu.CompilerParams(vmem_limit_bytes=8 * 2**20),
        name="finish",
    )(info, span, own, right, left)


def own_kernel(tokens, info, span, owner, rows_ref, out):
    members, forks = rows_ref.shape[:2]
    me = info[0]
    row = lax.rem(lax.broadcasted_iota(jnp.int32, (2 * tokens, HEAD_DIM), 0), tokens)
    for i in range(members):
        picked = jnp.zeros((2 * tokens, HEAD_DIM), jnp.float32)
        for f in range(forks):
            mine = (owner[f] == me) & (row + i * tokens < span[f])
            picked = jnp.where(mine, rows_ref[i, f].astype(jnp.float32), picked)
        out[i * tokens : (i + 1) * tokens, :HEAD_DIM] = picked[:tokens]
        out[i * tokens : (i + 1) * tokens, HEAD_DIM:] = picked[tokens:]


def own_kv(info, span, owner, q, tokens, width):
    members, forks, carried, _ = q.shape
    smem = pl.BlockSpec(memory_space=pltpu.SMEM)
    at = carried // (2 * tokens) - 1
    return pl.pallas_call(
        functools.partial(own_kernel, tokens),
        grid=(1,),
        in_specs=[smem] * 3
        + [pl.BlockSpec((members, forks, 2 * tokens, HEAD_DIM), lambda g: (0, 0, at, 0))],
        out_specs=pl.BlockSpec((members * tokens, width), lambda g: (0, 0)),
        out_shape=jax.ShapeDtypeStruct((members * tokens, width), jnp.float32),
        compiler_params=pltpu.CompilerParams(vmem_limit_bytes=8 * 2**20),
        name="own_kv",
    )(info, span, owner, q).astype(jnp.bfloat16)


def body(queries, tool_key_value, cache, placed, blocks, span_len, owner):
    forks, tokens, width = tool_key_value.shape
    heads = queries.shape[2] // HEAD_DIM
    rows = heads * tokens
    me = lax.axis_index("inst")
    members = lax.axis_size("inst")
    half = members // 2
    live = placed[:, 0] * blocks[:, 0] * BLOCK
    info = jnp.concatenate([me.astype(jnp.int32)[None], live])
    own_q = queries.reshape(forks, tokens, heads, HEAD_DIM).transpose(0, 2, 1, 3)
    fresh = tool_key_value.reshape(forks, tokens, 2, HEAD_DIM).transpose(0, 2, 1, 3)
    own_q, fresh = own_q.reshape(forks, rows, HEAD_DIM), fresh.reshape(forks, 2 * tokens, HEAD_DIM)
    sent = jnp.concatenate([own_q, fresh], axis=1).astype(jnp.float32) * WIDE
    q = lax.all_gather(sent.astype(jnp.float16), "inst", axis=0)
    q = (q.astype(jnp.float32) * (1.0 / WIDE)).astype(jnp.bfloat16)

    part = {}
    for offsets in CALLS(half):
        codes = tuple(o in (-half, half - 1) for o in offsets)
        got = parts_of(q, offsets, codes, info, cache, fresh, tokens)
        part.update(zip(offsets, got))

    left, right = part[-half], part[half - 1]
    for k in range(half - 1, 0, -1):
        left = passed_along(left, -1)
        right = passed_along(right, 1)
        (left,) = merge(left, part[-k])
        if k > 1:
            (right,) = merge(right, part[k - 1])
    left = passed_along(left, -1)
    owned = own_kv(info, span_len, owner, q, tokens, width).reshape(1, 1, members * tokens, width)
    attended = finish(info, span_len, part[0], right, left, tokens, rows)
    attended = attended.reshape(forks, heads, tokens, HEAD_DIM).transpose(0, 2, 1, 3)
    return attended.reshape(forks, tokens, heads * HEAD_DIM), owned


def CALLS(half):
    order = []
    for k in range(half, 0, -1):
        order += [-k, k - 1]
    return [tuple(order)]


def solution(mesh):
    return jax.shard_map(
        body,
        mesh=mesh,
        in_specs=(
            P(("groups", "rep"), "inst", "tp"),
            P(("groups", "rep"), "inst", "tp"),
            P(("groups", "rep"), "inst", "tp"),
            P(("groups", "rep"), "inst"),
            P(("groups", "rep"), "inst"),
            P(("groups", "rep")),
            P(("groups", "rep")),
        ),
        out_specs=(P(("groups", "rep"), "inst", "tp"), P(("groups", "inst"), "rep", None, "tp")),
        check_vma=False,
    )
```
